256 devices in a mesh: ep: 32 (over z, y), dp: 8 (over x, core).
Axes of the slice: x: 4, y: 4, z: 8, core: 2. Of those that a mesh axis runs over, the one named last changes fastest.
Arguments:
- act_in: bfloat16 [24576, 512], P(('ep', 'dp'))
- grad_out: bfloat16 [24576, 512], P(('ep', 'dp'))
- slot_ids: int32 [2, 24576, 8], P(None, ('ep', 'dp'))
- gate_vals: float32 [2, 24576, 8], P(None, ('ep', 'dp'))
- w_dense: bfloat16 [2, 512, 512], replicated
- w_gate: bfloat16 [2, 128, 512, 176], P(None, 'ep')
- w_up: bfloat16 [2, 128, 512, 176], P(None, 'ep')
- w_down: bfloat16 [2, 128, 176, 512], P(None, 'ep')
- ws_gate: bfloat16 [2, 512, 176], replicated
- ws_up: bfloat16 [2, 512, 176], replicated
- ws_down: bfloat16 [2, 176, 512], replicated
Outputs:
- output 1: bfloat16 [24576, 512], P(('ep', 'dp'))
- output 2: bfloat16 [2, 512, 512], replicated
- output 3: bfloat16 [2, 128, 512, 176], P(None, 'ep')
- output 4: bfloat16 [2, 128, 512, 176], P(None, 'ep')
- output 5: bfloat16 [2, 128, 176, 512], P(None, 'ep')
- output 6: bfloat16 [2, 512, 176], replicated
- output 7: bfloat16 [2, 512, 176], replicated
- output 8: bfloat16 [2, 176, 512], replicated
All inputs are finite; a program needn't handle non-finite values.
Results may differ from the reference program's by a relative error of at most 0.02.
Values are sent between devices in bfloat16 or wider.
A program may use at most 768 MiB of HBM per device.

```python
import functools
import jax
import jax.numpy as jnp
from jax import lax

D = 512
FF = 176
FS = 176
EXPERTS = 128
TOP = 8
TOKENS = 96
EP = 32
DP = 8
LAYERS = 2

NUM_DEV = EP * DP
CAP = 2 * TOKENS * TOP // EXPERTS
ROWS = NUM_DEV * TOKENS


def draw_slots(key):
    key_tok, key_exp = jax.random.split(key)
    mean_load = TOKENS * TOP // EXPERTS
    order = jax.random.permutation(key_tok, TOKENS)
    position = jnp.arange(TOP, dtype=jnp.int32)[None, :] * TOKENS + order[:, None]
    group = position // (4 * mean_load)
    rest = position % (4 * mean_load)
    first = 2 * mean_load
    second = first + mean_load // 2
    third = second + mean_load // 2
    within = (rest >= first).astype(jnp.int32) + (rest >= second).astype(jnp.int32) + (rest >= third).astype(jnp.int32)
    start = jnp.where(rest >= third, third, jnp.where(rest >= second, second, jnp.where(rest >= first, first, 0)))
    expert_perm = jax.random.permutation(key_exp, EXPERTS)
    expert = expert_perm[group * 4 + within]
    return (expert * CAP + rest - start).astype(jnp.int32)


def setup_inputs(seed: int = 0) -> dict:
    keys = jax.random.split(jax.random.key(seed), 12)
    slot_keys = jax.random.split(keys[0], LAYERS * NUM_DEV)
    slot_ids = jax.vmap(draw_slots)(slot_keys).reshape(LAYERS, ROWS, TOP)
    gate_vals = jax.random.uniform(keys[1], (LAYERS, ROWS, TOP), jnp.float32, 0.5, 1.5) / TOP
    act_in = jax.random.normal(keys[2], (ROWS, D), jnp.float32).astype(jnp.bfloat16)
    grad_out = jax.random.normal(keys[3], (ROWS, D), jnp.float32).astype(jnp.bfloat16)
    w_dense = (jax.random.normal(keys[4], (LAYERS, D, D), jnp.float32) * D ** -0.5).astype(jnp.bfloat16)
    w_gate = (jax.random.normal(keys[5], (LAYERS, EXPERTS, D, FF), jnp.float32) * D ** -0.5).astype(jnp.bfloat16)
    w_up = (jax.random.normal(keys[6], (LAYERS, EXPERTS, D, FF), jnp.float32) * D ** -0.5).astype(jnp.bfloat16)
    w_down = (jax.random.normal(keys[7], (LAYERS, EXPERTS, FF, D), jnp.float32) * FF ** -0.5).astype(jnp.bfloat16)
    ws_gate = (jax.random.normal(keys[8], (LAYERS, D, FS), jnp.float32) * D ** -0.5).astype(jnp.bfloat16)
    ws_up = (jax.random.normal(keys[9], (LAYERS, D, FS), jnp.float32) * D ** -0.5).astype(jnp.bfloat16)
    ws_down = (jax.random.normal(keys[10], (LAYERS, FS, D), jnp.float32) * FS ** -0.5).astype(jnp.bfloat16)
    return {"act_in": act_in, "grad_out": grad_out, "slot_ids": slot_ids, "gate_vals": gate_vals, "w_dense": w_dense, "w_gate": w_gate, "w_up": w_up, "w_down": w_down, "ws_gate": ws_gate, "ws_up": ws_up, "ws_down": ws_down}


def expert_block(args, w_gate32, w_up32, w_down32):
    mixed_loc, slot_loc, gate_loc = args
    slot_flat = slot_loc.reshape(TOKENS * TOP)
    copies = jnp.broadcast_to(mixed_loc[:, None, :], (TOKENS, TOP, D)).reshape(TOKENS * TOP, D)
    dispatched = jnp.zeros((EXPERTS * CAP, D), mixed_loc.dtype).at[slot_flat].set(copies)
    dispatched = dispatched.reshape(EXPERTS, CAP, D).astype(jnp.float32)
    a_one = jnp.einsum("ecd,edf->ecf", dispatched, w_gate32)
    a_three = jnp.einsum("ecd,edf->ecf", dispatched, w_up32)
    hidden = (jax.nn.silu(a_one) * a_three).astype(jnp.bfloat16)
    exp_out = jnp.einsum("ecf,efd->ecd", hidden.astype(jnp.float32), w_down32).astype(jnp.bfloat16)
    picked = exp_out.reshape(EXPERTS * CAP, D)[slot_flat].reshape(TOKENS, TOP, D)
    return jnp.sum(gate_loc[:, :, None] * picked.astype(jnp.float32), axis=1)


def moe_layer(act, layer_in):
    w_dense, w_gate, w_up, w_down, ws_gate, ws_up, ws_down, slot_ids, gate_vals = layer_in
    dense_pre = jnp.dot(act, w_dense, preferred_element_type=jnp.float32)
    mixed = (act.astype(jnp.float32) + dense_pre).astype(jnp.bfloat16)
    s_one = jnp.dot(mixed, ws_gate, preferred_element_type=jnp.float32)
    s_three = jnp.dot(mixed, ws_up, preferred_element_type=jnp.float32)
    shared_hidden = (jax.nn.silu(s_one) * s_three).astype(jnp.bfloat16)
    shared_out = jnp.dot(shared_hidden, ws_down, preferred_element_type=jnp.float32)
    block = jax.checkpoint(functools.partial(expert_block, w_gate32=w_gate.astype(jnp.float32), w_up32=w_up.astype(jnp.float32), w_down32=w_down.astype(jnp.float32)))
    routed = lax.map(block, (mixed.reshape(NUM_DEV, TOKENS, D), slot_ids.reshape(NUM_DEV, TOKENS, TOP), gate_vals.reshape(NUM_DEV, TOKENS, TOP)))
    routed = routed.reshape(ROWS, D)
    new_act = (mixed.astype(jnp.float32) + routed + shared_out).astype(jnp.bfloat16)
    return new_act, None


def reference(act_in, grad_out, slot_ids, gate_vals, w_dense, w_gate, w_up, w_down, ws_gate, ws_up, ws_down):
    def forward(act, dense_all, gate_all, up_all, down_all, sgate_all, sup_all, sdown_all):
        final, _ = lax.scan(moe_layer, act, (dense_all, gate_all, up_all, down_all, sgate_all, sup_all, sdown_all, slot_ids, gate_vals))
        return final
    _, pullback = jax.vjp(forward, act_in, w_dense, w_gate, w_up, w_down, ws_gate, ws_up, ws_down)
    grads = pullback(grad_out)
    return (grads[0], grads[1], grads[2], grads[3], grads[4], grads[5], grads[6], grads[7])
```

```python
import functools
import jax
import jax.numpy as jnp
from jax import lax
from jax.experimental import pallas as pl
from jax.experimental.pallas import tpu as pltpu
from jax.sharding import PartitionSpec as P

ALL_AXES = ("ep", "dp")
MESH = pl.DeviceIdType.MESH
F32 = jnp.float32
BF16 = jnp.bfloat16
NY = 4
LOCAL_EXP = 4
INFO_ROWS = 16
FIRST_ROWS = 64
LANES = 128


def nn(a, b):
    return lax.dot_general(a, b, (((1,), (0,)), ((), ())), preferred_element_type=F32)


def nt(a, b):
    return lax.dot_general(a, b, (((1,), (1,)), ((), ())), preferred_element_type=F32)


def tn(a, b):
    return lax.dot_general(a, b, (((0,), (0,)), ((), ())), preferred_element_type=F32)


def sigmoid(a):
    return 1.0 / (1.0 + jnp.exp(-a))


def split3(value):
    high = value.astype(BF16)
    rest = value - high.astype(F32)
    mid = rest.astype(BF16)
    low = (rest - mid.astype(F32)).astype(BF16)
    return high, mid, low


def ring_span(size, even):
    plus, minus = size // 2, (size - 1) // 2
    return range(-minus, plus + 1) if even else range(-plus, minus + 1)


def sign(v):
    return (v > 0) - (v < 0)


def gather_plan(nz, ny):
    nodes = []
    for kz in ring_span(nz, True):
        for ky in ring_span(ny, kz % 2 == 0):
            nodes.append((0, kz, ky))
    for ky in ring_span(ny, True):
        for kz in ring_span(nz, ky % 2 == 0):
            nodes.append((1, kz, ky))
    nodes = [n for n in nodes if n[1] or n[2]]
    nodes.sort(key=lambda n: abs(n[1]) + abs(n[2]))
    return nodes


def parent_of(node):
    part, kz, ky = node
    if part == 0:
        return (part, kz, ky - sign(ky)) if ky else (part, kz - sign(kz), 0)
    return (part, kz - sign(kz), ky) if kz else (part, 0, ky - sign(ky))


class Gather:
    def __init__(self, buf, splits, send, recv, me, nz, dp):
        self.buf, self.splits, self.send, self.recv = buf, splits, send, recv
        self.nz, self.dp = nz, dp
        self.z, self.y = me // NY, me % NY
        self.nodes = gather_plan(nz, NY)
        self.ids = {node: i for i, node in enumerate(self.nodes)}
        self.children = {}
        for node in self.nodes:
            self.children.setdefault(parent_of(node), []).append(node)

    def ep_at(self, dz, dy):
        return ((self.z + dz + 2 * self.nz) % self.nz) * NY + (self.y + dy + 2 * NY) % NY

    def block(self, part, kz, ky):
        low, high = self.splits[part], self.splits[part + 1]
        return self.buf.at[self.ep_at(-kz, -ky), pl.ds(low, high - low)]

    def out_copy(self, node):
        part, pz, py = parent_of(node)
        ref = self.block(part, pz, py)
        i = self.ids[node]
        target = self.ep_at(node[1] - pz, node[2] - py)
        return pltpu.make_async_remote_copy(src_ref=ref, dst_ref=ref, send_sem=self.send.at[i], recv_sem=self.recv.at[i], device_id=(target, self.dp), device_id_type=MESH)

    def in_copy(self, node):
        part, pz, py = parent_of(node)
        ref = self.block(*node)
        i = self.ids[node]
        source = self.ep_at(pz - node[1], py - node[2])
        return pltpu.make_async_remote_copy(src_ref=ref, dst_ref=ref, send_sem=self.send.at[i], recv_sem=self.recv.at[i], device_id=(source, self.dp), device_id_type=MESH)

    def begin(self):
        for part in (0, 1):
            for child in self.children[(part, 0, 0)]:
                self.out_copy(child).start()

    def rounds(self):
        by_hops = {}
        for node in self.nodes:
            by_hops.setdefault(abs(node[1]) + abs(node[2]), []).append(node)
        return [by_hops[h] for h in sorted(by_hops)]

    def advance(self, nodes):
        for node in nodes:
            self.in_copy(node).wait_recv()
            for child in self.children.get(node, ()):
                self.out_copy(child).start()

    def finish(self):
        for node in self.nodes:
            self.out_copy(node).wait_send()


class Exchange:
    def __init__(self, src, dst, send, recv, me, nz, dp):
        self.src, self.dst, self.send, self.recv, self.nz, self.dp, self.me = src, dst, send, recv, nz, dp, me
        self.z, self.y = me // NY, me % NY

    def ep_at(self, dz, dy):
        return ((self.z + dz + self.nz) % self.nz) * NY + (self.y + dy + NY) % NY

    def order(self):
        half = []
        for k in range(1, self.nz // 2 + 1):
            half += [k] if 2 * k == self.nz else [k, self.nz - k]
        return half + [0]

    def copy(self, dz, dy, peer, block, slot):
        i = dz * NY + dy
        return pltpu.make_async_remote_copy(src_ref=self.src.at[block], dst_ref=self.dst.at[slot], send_sem=self.send.at[i], recv_sem=self.recv.at[i], device_id=(peer, self.dp), device_id_type=MESH)

    def start(self, dz):
        for dy in range(NY):
            if dz or dy:
                peer = self.ep_at(dz, dy)
                self.copy(dz, dy, peer, peer, self.me).start()
        if dz == 0:
            self.dst[self.me] = self.src[self.me]

    def wait_all(self):
        for dz in self.order():
            for dy in range(NY):
                if dz or dy:
                    peer = self.ep_at(-dz, -dy)
                    self.copy(dz, dy, peer, peer, peer).wait_recv()

    def finish(self):
        for dz in range(self.nz):
            for dy in range(NY):
                if dz or dy:
                    peer = self.ep_at(dz, dy)
                    self.copy(dz, dy, peer, peer, self.me).wait_send()


def enter(me, ep, dp):
    barrier = pltpu.get_barrier_semaphore()

    def hello(off, carry):
        pl.semaphore_signal(barrier, inc=1, device_id=((me + off) % ep, dp), device_id_type=MESH)
        return carry

    lax.fori_loop(1, ep, hello, 0)
    pl.semaphore_wait(barrier, ep - 1)


def info_block(slots, gates):
    top, tokens = slots.shape
    high_slot = slots // 16
    low_slot = slots - high_slot * 16
    high, mid, low = split3(gates)
    pad = jnp.zeros((top, LANES - tokens), BF16)

    def wide(rows):
        return jnp.concatenate([rows, pad], axis=1)

    upper = jnp.concatenate([wide(high_slot.astype(F32).astype(BF16)), wide(low_slot.astype(F32).astype(BF16)), wide(high), wide(mid)], axis=1)
    lower = jnp.concatenate([wide(low), jnp.zeros((top, 3 * LANES), BF16)], axis=1)
    return upper, lower


def build_select(s_group, info_ref, tgt_ref, first_slot, select_ref, gate_ref, top, per_exp):
    rows = LOCAL_EXP * NY * per_exp
    row_gate = jnp.zeros((rows, 1), F32)
    for si in range(NY):
        src = s_group * NY + si
        info = info_ref[src].astype(F32)
        slot = info[0:top, 0:LANES] * 16.0 + info[0:top, LANES:2 * LANES]
        gate = info[0:top, 2 * LANES:3 * LANES] + info[0:top, 3 * LANES:4 * LANES] + info[8:8 + top, 0:LANES]
        slot = slot - first_slot
        lane = lax.broadcasted_iota(jnp.int32, slot.shape, 1)
        slot = jnp.where(lane < 96, slot, -2000000.0)
        target = tgt_ref[si]
        found = jnp.full((rows, LANES), -1.0, F32)
        for j in range(top):
            found = jnp.where(slot[j:j + 1, :] == target, gate[j:j + 1, :], found)
        select_ref[src] = jnp.where(found >= 0.0, 1.0, 0.0).astype(BF16)
        row_gate = row_gate + jnp.sum(jnp.maximum(found, 0.0), axis=1, keepdims=True)
    gate_ref[s_group] = jnp.broadcast_to(row_gate, (rows, LANES))


def init_targets(tgt_ref, perm_ref, per_exp):
    rows = LOCAL_EXP * NY * per_exp
    row = lax.broadcasted_iota(jnp.int32, (rows, LANES), 0)
    expert = row // (NY * per_exp)
    rest = row - expert * (NY * per_exp)
    source = rest // per_exp
    slot = expert * per_exp + rest - source * per_exp
    for si in range(NY):
        tgt_ref[si] = jnp.where(source == si, slot, -1000000).astype(F32)
    out_row = lax.broadcasted_iota(jnp.int32, (rows, rows), 0)
    in_row = lax.broadcasted_iota(jnp.int32, (rows, rows), 1)
    out_source = out_row // (LOCAL_EXP * per_exp)
    out_rest = out_row - out_source * (LOCAL_EXP * per_exp)
    out_expert = out_rest // per_exp
    wanted = out_expert * (NY * per_exp) + out_source * per_exp + out_rest - out_expert * per_exp
    perm_ref[...] = jnp.where(in_row == wanted, 1.0, 0.0).astype(BF16)


def expand(s_group, select_ref, block_ref, tokens):
    total = None
    for si in range(NY):
        src = s_group * NY + si
        part = nn(select_ref[src][:, :tokens], block_ref[src, 0:tokens])
        total = part if total is None else total + part
    return total


def scatter_rows(s_group, rows32, dst_ref, per_exp):
    size = NY * per_exp
    values = rows32.astype(BF16)
    for e in range(LOCAL_EXP):
        dst_ref[e, pl.ds(pl.multiple_of(s_group * size, 16), size)] = values[e * size:(e + 1) * size]


def permute_group(s_group, src_ref, perm_ref, out_ref, per_exp):
    size = NY * per_exp
    rows = jnp.concatenate([src_ref[e, pl.ds(pl.multiple_of(s_group * size, 16), size)] for e in range(LOCAL_EXP)], axis=0)
    mixed = nn(perm_ref[...], rows).astype(BF16)
    for si in range(NY):
        out_ref[s_group * NY + si] = mixed[si * LOCAL_EXP * per_exp:(si + 1) * LOCAL_EXP * per_exp]


def slot_matrix(slot_cols, gate_cols, dst_ref, tokens, top, n_slots):
    step = 3 * LANES
    for c in range(n_slots // step):
        lane = (lax.broadcasted_iota(jnp.int32, (tokens, step), 1) + c * step).astype(F32)
        found = jnp.zeros((tokens, step), F32)
        for j in range(top):
            value = 1.0 if gate_cols is None else gate_cols[:, j:j + 1]
            found = jnp.where(slot_cols[:, j:j + 1] == lane, value, found)
        cols = pl.ds(c * step, step)
        if gate_cols is None:
            dst_ref[:, cols] = found.astype(BF16)
        else:
            for k, piece in enumerate(split3(found)):
                dst_ref[k * tokens:(k + 1) * tokens, cols] = piece


def forward_kernel(dims, x_ref, dy_ref, slots_ref, gates_ref, slot_cols_ref, gate_cols_ref, wd_ref, w1_hbm, w3_hbm, w2_hbm, ws1_ref, ws3_ref, ws2_ref,
                   u_out, rows_out, select_out, gate_out, dy_all, x2_out,
                   u_all, w1, w3, w2, tgt, perm, exp_out, send_buf, recv_buf, slot_mat, gsend, grecv, dsend, drecv, asend, arecv, wsem):
    ep, tokens, top, per_exp = dims
    nz = ep // NY
    me, dp = lax.axis_index("ep"), lax.axis_index("dp")
    loads = [pltpu.make_async_copy(h, v, wsem.at[i]) for i, (h, v) in enumerate([(w1_hbm, w1), (w3_hbm, w3), (w2_hbm, w2)])]
    for load in loads:
        load.start()
    x = x_ref[...]
    u32 = x.astype(F32) + nn(x, wd_ref[...])
    u = u32.astype(BF16)
    u_all[me, 0:tokens] = u
    upper, lower = info_block(slots_ref[0], gates_ref[0])
    u_all[me, tokens:tokens + top] = upper
    u_all[me, tokens + 8:tokens + 8 + top] = lower
    u_out[...] = u
    dy_all[me, 0:tokens] = dy_ref[...]
    upper, lower = info_block(slots_ref[1], gates_ref[1])
    dy_all[me, tokens:tokens + top] = upper
    dy_all[me, tokens + 8:tokens + 8 + top] = lower
    enter(me, ep, dp)
    splits = (0, FIRST_ROWS, tokens + INFO_ROWS)
    gather = Gather(u_all, splits, gsend, grecv, me, nz, dp)
    gather.begin()
    init_targets(tgt, perm, per_exp)
    slot_matrix(slot_cols_ref[...], gate_cols_ref[...], slot_mat, tokens, top, ep * LOCAL_EXP * per_exp)
    for nodes in gather.rounds():
        gather.advance(nodes)
    late = Gather(dy_all, splits, dsend, drecv, me, nz, dp)
    late.begin()
    first_slot = (me * (LOCAL_EXP * per_exp)).astype(F32)

    def fill(g, carry):
        build_select(g, u_all.at[:, pl.ds(tokens, INFO_ROWS)], tgt, first_slot, select_out, gate_out, top, per_exp)
        scatter_rows(g, expand(g, select_out, u_all, tokens), rows_out, per_exp)
        return carry

    lax.fori_loop(0, nz, fill, 0)
    for load in loads:
        load.wait()

    def experts(e, carry):
        rows = rows_out[e]
        a_one = nt(rows, w1[e])
        a_three = nt(rows, w3[e])
        hidden = (a_one * sigmoid(a_one) * a_three).astype(BF16)
        exp_out[e] = nn(hidden, w2[e]).astype(BF16)
        return carry

    lax.fori_loop(0, LOCAL_EXP, experts, 0)
    back = Exchange(send_buf, recv_buf, asend, arecv, me, nz, dp)
    for dz in back.order():
        permute_group((back.z + dz) % nz, exp_out, perm, send_buf, per_exp)
        back.start(dz)
    s_one = nt(u, ws1_ref[...])
    s_three = nt(u, ws3_ref[...])
    shared_hidden = (s_one * sigmoid(s_one) * s_three).astype(BF16)
    base = u.astype(F32) + nn(shared_hidden, ws2_ref[...])
    for nodes in late.rounds():
        late.advance(nodes)
    back.wait_all()
    picked = nn(slot_mat[...], recv_buf[...].reshape(ep * LOCAL_EXP * per_exp, recv_buf.shape[2]))
    routed = picked[0:tokens] + picked[tokens:2 * tokens] + picked[2 * tokens:3 * tokens]
    x2_out[...] = (base + routed).astype(BF16)
    gather.finish()
    late.finish()
    back.finish()


def backward_kernel(dims, second, *refs):
    ep, tokens, top, per_exp = dims
    nz = ep // NY
    if second:
        (x_ref, dy_ref, slot_cols_ref, wd_ref, w1_hbm, w3_hbm, w2_hbm, ws1_ref, ws3_ref, ws2_ref, dy_all,
         dx_out, g_wd, g_w1, g_w3, g_w2, g_ws1, g_ws3, g_ws2,
         rows, gate, select, block_all, w1, w3, w2, tgt, perm, grad_rows, exp_out, send_buf, recv_buf, slot_mat, gsend, grecv, asend, arecv, wsem) = refs
    else:
        (x_ref, dy_ref, slot_cols_ref, wd_ref, w1_hbm, w3_hbm, w2_hbm, ws1_ref, ws3_ref, ws2_ref, u_ref, rows, gate, select,
         dx_out, g_wd, g_w1, g_w3, g_w2, g_ws1, g_ws3, g_ws2,
         block_all, w1, w3, w2, tgt, perm, grad_rows, exp_out, send_buf, recv_buf, slot_mat, gsend, grecv, asend, arecv, wsem) = refs
    me, dp = lax.axis_index("ep"), lax.axis_index("dp")
    loads = [pltpu.make_async_copy(h, v, wsem.at[i]) for i, (h, v) in enumerate([(w1_hbm, w1), (w3_hbm, w3), (w2_hbm, w2)])]
    for load in loads:
        load.start()
    x = x_ref[...]
    dy = dy_ref[...]
    if second:
        u = (x.astype(F32) + nn(x, wd_ref[...])).astype(BF16)
        block_all[me] = u
    else:
        u = u_ref[...]
        block_all[me] = dy
    enter(me, ep, dp)
    gather = Gather(block_all, (0, FIRST_ROWS, tokens), gsend, grecv, me, nz, dp)
    gather.begin()
    init_targets(tgt, perm, per_exp)
    slot_matrix(slot_cols_ref[...], None, slot_mat, tokens, top, ep * LOCAL_EXP * per_exp)
    first_slot = (me * (LOCAL_EXP * per_exp)).astype(F32)

    def gated(g, source_ref):
        rows32 = expand(g, select, source_ref, tokens)
        scale = jnp.concatenate([gate[g]] * (rows32.shape[1] // LANES), axis=1)
        scatter_rows(g, rows32 * scale, grad_rows, per_exp)

    def early(g, carry):
        build_select(g, dy_all.at[:, pl.ds(tokens, INFO_ROWS)], tgt, first_slot, select, gate, top, per_exp)
        gated(g, dy_all)
        return carry

    rounds = gather.rounds()
    share = -(-nz // len(rounds))
    for i, nodes in enumerate(rounds):
        gather.advance(nodes)
        if second:
            low, high = min(i * share, nz), min((i + 1) * share, nz)
            if high > low:
                lax.fori_loop(low, high, early, 0)

    def fill(g, carry):
        if second:
            scatter_rows(g, expand(g, select, block_all, tokens), rows, per_exp)
        else:
            gated(g, block_all)
        return carry

    lax.fori_loop(0, nz, fill, 0)
    for load in loads:
        load.wait()

    def experts(e, carry):
        x_rows = rows[e]
        g_rows = grad_rows[e]
        a_one = nt(x_rows, w1[e])
        a_three = nt(x_rows, w3[e])
        sig = sigmoid(a_one)
        silu = a_one * sig
        hidden = (silu * a_three).astype(BF16)
        g_hidden = nt(g_rows, w2[e])
        g_one = (g_hidden * a_three * (sig * (1.0 + a_one * (1.0 - sig)))).astype(BF16)
        g_three = (g_hidden * silu).astype(BF16)
        exp_out[e] = (nn(g_one, w1[e]) + nn(g_three, w3[e])).astype(BF16)
        g_w1[e] = tn(g_one, x_rows).astype(BF16)
        g_w3[e] = tn(g_three, x_rows).astype(BF16)
        g_w2[e] = tn(hidden, g_rows).astype(BF16)
        return carry

    lax.fori_loop(0, LOCAL_EXP, experts, 0)
    back = Exchange(send_buf, recv_buf, asend, arecv, me, nz, dp)
    for dz in back.order():
        permute_group((back.z + dz) % nz, exp_out, perm, send_buf, per_exp)
        back.start(dz)
    s_one = nt(u, ws1_ref[...])
    s_three = nt(u, ws3_ref[...])
    sig = sigmoid(s_one)
    silu = s_one * sig
    shared_hidden = (silu * s_three).astype(BF16)
    g_ws2[...] = tn(shared_hidden, dy).astype(BF16)
    g_shared = nt(dy, ws2_ref[...])
    g_one = (g_shared * s_three * (sig * (1.0 + s_one * (1.0 - sig)))).astype(BF16)
    g_three = (g_shared * silu).astype(BF16)
    g_ws1[...] = tn(g_one, u).astype(BF16)
    g_ws3[...] = tn(g_three, u).astype(BF16)
    base = dy.astype(F32) + nn(g_one, ws1_ref[...]) + nn(g_three, ws3_ref[...])
    back.wait_all()
    routed = nn(slot_mat[...], recv_buf[...].reshape(ep * LOCAL_EXP * per_exp, recv_buf.shape[2]))
    g_mixed = (base + routed).astype(BF16)
    dx_out[...] = (g_mixed.astype(F32) + nt(g_mixed, wd_ref[...])).astype(BF16)
    g_wd[...] = tn(x, g_mixed).astype(BF16)
    gather.finish()
    back.finish()


def vmem():
    return pl.BlockSpec(memory_space=pltpu.VMEM)


def hbm():
    return pl.BlockSpec(memory_space=pl.ANY)


def params(cid):
    return pltpu.CompilerParams(collective_id=cid, has_side_effects=True, vmem_limit_bytes=60 * 1024 * 1024)


def comm_sems(ep, gathers):
    hops = 2 * (ep - 1)
    dma = pltpu.SemaphoreType.DMA
    return [dma((hops,)) for _ in range(2 * gathers)] + [dma((ep,)), dma((ep,)), dma((3,))]


def forward_layer(ep, x, dy, slots, gates, slot_cols, gate_cols, weights):
    wd, w1, w3, w2, ws1, ws3, ws2 = weights
    tokens, width = x.shape
    top = slots.shape[1]
    hid = w1.shape[1]
    per_exp = 2 * tokens * top // (LOCAL_EXP * ep)
    nz = ep // NY
    group = LOCAL_EXP * NY * per_exp
    sds = jax.ShapeDtypeStruct
    outs = [
        sds((tokens, width), BF16),
        sds((LOCAL_EXP, ep * per_exp, width), BF16),
        sds((ep, group, LANES), BF16),
        sds((nz, group, LANES), F32),
        sds((ep, tokens + INFO_ROWS, width), BF16),
        sds((tokens, width), BF16),
    ]
    v = pltpu.VMEM
    scratch = [
        v((ep, tokens + INFO_ROWS, width), BF16),
        v((LOCAL_EXP, hid, width), BF16), v((LOCAL_EXP, hid, width), BF16), v((LOCAL_EXP, hid, width), BF16),
        v((NY, group, LANES), F32), v((group, group), BF16),
        v((LOCAL_EXP, ep * per_exp, width), BF16),
        v((ep, LOCAL_EXP * per_exp, width), BF16), v((ep, LOCAL_EXP * per_exp, width), BF16),
        v((3 * tokens, ep * LOCAL_EXP * per_exp), BF16),
    ] + comm_sems(ep, 2)
    return pl.pallas_call(
        functools.partial(forward_kernel, (ep, tokens, top, per_exp)),
        out_shape=outs,
        in_specs=[vmem()] * 7 + [hbm()] * 3 + [vmem()] * 3,
        out_specs=[vmem()] * 6,
        scratch_shapes=scratch,
        compiler_params=params(0),
        name="forward_layer",
    )(x, dy, slots, gates, slot_cols, gate_cols, wd, w1, w3, w2, ws1, ws3, ws2)


def backward_layer(ep, cid, second, x, dy, slot_cols, weights, extra):
    wd, w1, w3, w2, ws1, ws3, ws2 = weights
    tokens, width = x.shape
    top = slot_cols.shape[1]
    hid = w1.shape[1]
    shid = ws1.shape[0]
    per_exp = 2 * tokens * top // (LOCAL_EXP * ep)
    nz = ep // NY
    group = LOCAL_EXP * NY * per_exp
    sds = jax.ShapeDtypeStruct
    outs = [sds((tokens, width), BF16), sds((width, width), BF16)] + [sds((LOCAL_EXP, hid, width), BF16)] * 3 + [sds((shid, width), BF16)] * 3
    v = pltpu.VMEM
    row_buf = v((LOCAL_EXP, ep * per_exp, width), BF16)
    scratch = [row_buf, v((nz, group, LANES), F32), v((ep, group, LANES), BF16)] if second else []
    scratch += [
        v((ep, tokens, width), BF16),
        v((LOCAL_EXP, hid, width), BF16), v((LOCAL_EXP, hid, width), BF16), v((LOCAL_EXP, hid, width), BF16),
        v((NY, group, LANES), F32), v((group, group), BF16),
        row_buf, row_buf,
        v((ep, LOCAL_EXP * per_exp, width), BF16), v((ep, LOCAL_EXP * per_exp, width), BF16),
        v((tokens, ep * LOCAL_EXP * per_exp), BF16),
    ] + comm_sems(ep, 1)
    return pl.pallas_call(
        functools.partial(backward_kernel, (ep, tokens, top, per_exp), second),
        out_shape=outs,
        in_specs=[vmem()] * 4 + [hbm()] * 3 + [vmem()] * (3 + len(extra)),
        out_specs=[vmem()] * 8,
        scratch_shapes=scratch,
        compiler_params=params(cid),
        name="backward_second" if second else "backward_first",
    )(x, dy, slot_cols, wd, w1, w3, w2, ws1, ws3, ws2, *extra)


def solution(mesh):
    ep = mesh.shape["ep"]
    tok_spec = P(ALL_AXES, None)
    route_spec = P(None, ALL_AXES, None)
    exp_spec = P(None, "ep", None, None)
    repl_spec = P(None, None, None)

    def body(act_in, grad_out, slot_ids, gate_vals, w_dense, w_gate, w_up, w_down, ws_gate, ws_up, ws_down):
        flip = functools.partial(jnp.swapaxes, axis1=-1, axis2=-2)
        w1t, w3t, ws1t, ws3t = flip(w_gate), flip(w_up), flip(ws_gate), flip(ws_up)
        weights = [(w_dense[k], w1t[k], w3t[k], w_down[k], ws1t[k], ws3t[k], ws_down[k]) for k in range(2)]
        slot_cols = slot_ids.astype(F32)
        u_one, rows, select, gate, dy_all, act_two = forward_layer(ep, act_in, grad_out, flip(slot_ids), flip(gate_vals), slot_cols[0], gate_vals[0], weights[0])
        two = backward_layer(ep, 1, True, act_two, grad_out, slot_cols[1], weights[1], (dy_all,))
        one = backward_layer(ep, 2, False, act_in, two[0], slot_cols[0], weights[0], (u_one, rows, gate, select))
        sums = []
        for part in (two, one):
            dense = [lax.psum(part[k], ALL_AXES) for k in (1, 5, 6, 7)]
            experts = [lax.psum(part[k], "dp") for k in (2, 3, 4)]
            sums.append((dense, experts))
        dense = [jnp.stack([sums[1][0][k], sums[0][0][k]]) for k in range(4)]
        experts = [jnp.stack([sums[1][1][k], sums[0][1][k]]) for k in range(3)]
        return (one[0], dense[0], flip(experts[0]), flip(experts[1]), experts[2], flip(dense[1]), flip(dense[2]), dense[3])

    return jax.shard_map(body, mesh=mesh, in_specs=(tok_spec, tok_spec, route_spec, route_spec, repl_spec, exp_spec, exp_spec, exp_spec, repl_spec, repl_spec, repl_spec), out_specs=(tok_spec, repl_spec, exp_spec, exp_spec, exp_spec, repl_spec, repl_spec, repl_spec), check_vma=False)
```
